32 devices in a mesh: dev: 32 (over z, y, x, core).
Axes of the slice: x: 2, y: 2, z: 4, core: 2. Of those that a mesh axis runs over, the one named last changes fastest.
Arguments:
- state_real: float32 [4194304], P('dev'), may hold values from -24 to 24, as said below
- state_imag: float32 [4194304], P('dev'), may hold values from -24 to 24, as said below
- subsystem: int32 [3], replicated, may hold values from 0 to 16, as said below
Outputs:
- rho_real: float32 [256, 256], P('dev')
- rho_imag: float32 [256, 256], P('dev')
The draws below stay inside these ranges and needn't reach their ends.
Inputs may be any that keep to these rules, and one draw needn't show every extreme that they name: `subsystem`: the 3 entries are distinct local bit positions in ascending order; the first is always 0 and the last always 17 - 1. `state_real`: real parts of amplitudes; their typical size changes between aligned blocks of 2**(11) local indices by up to a factor of 16. `state_imag`: imaginary parts of amplitudes, with the same block sizes as the real parts.
All inputs are finite; a program needn't handle non-finite values.
Results may differ from the reference program's by a relative error of at most 0.0001.
Values sent between devices are 32-bit elements; how exact they have to be, the bound alone decides.
A program may use at most 192 MiB of HBM per device.

```python
import jax
import jax.numpy as jnp
from jax import lax

LOCAL_QUBITS = 17
SUB_LOCAL = 3
AMPS_DEV = 131072
AMPS = 4194304
COMPLEMENT = 16384
SUB_DIM = 256
N_DEV = 32


def amplitude_envelope(key):
    block_total = AMPS // 2 ** (LOCAL_QUBITS - 6)
    levels = jax.random.uniform(jax.random.fold_in(key, 11), (block_total,), jnp.float32, -1.3862943611198906, 1.3862943611198906)
    return jnp.repeat(jnp.exp(levels), AMPS // block_total, total_repeat_length=AMPS)


def draw_noise(key, salt_value):
    noise_key = jax.random.fold_in(key, salt_value)
    return jnp.clip(jax.random.normal(noise_key, (AMPS,), jnp.float32), -6.0, 6.0)


def draw_state_real(key, part):
    return (amplitude_envelope(key) * draw_noise(key, 3)).astype(jnp.float32)


def draw_state_imag(key, part):
    return (amplitude_envelope(key) * draw_noise(key, 5)).astype(jnp.float32)


def draw_subsystem(key, part):
    middle = jax.random.randint(jax.random.fold_in(key, 17), (1,), 1, LOCAL_QUBITS - 1, jnp.int32)
    lowest = jnp.zeros((1,), jnp.int32)
    highest = jnp.full((1,), LOCAL_QUBITS - 1, jnp.int32)
    return jnp.concatenate([lowest, middle, highest]).astype(jnp.int32)


def setup_inputs(seed: int = 0) -> dict:
    arg_keys = jax.random.split(jax.random.key(seed), 4)
    state_real = draw_state_real(jax.random.fold_in(arg_keys[3], 71), 0)
    state_imag = draw_state_imag(jax.random.fold_in(arg_keys[3], 71), 0)
    subsystem = draw_subsystem(jax.random.fold_in(arg_keys[3], 71), 0)
    return dict(state_real=state_real, state_imag=state_imag, subsystem=subsystem)


def insert_bits(subsystem, count_sub, count_rest):
    picked = lax.broadcasted_iota(jnp.int32, (count_sub, count_rest), 0)
    source = lax.broadcasted_iota(jnp.int32, (count_sub, count_rest), 1)
    for sub_index in range(subsystem.shape[0]):
        bit_place = subsystem[sub_index].astype(jnp.int32)
        lower_bits = jnp.bitwise_and(source, jnp.left_shift(jnp.int32(1), bit_place) - jnp.int32(1))
        upper_bits = jnp.left_shift(jnp.right_shift(source, bit_place), bit_place + jnp.int32(1))
        chosen_bit = jnp.left_shift(jnp.bitwise_and(jnp.right_shift(picked, sub_index), jnp.int32(1)), bit_place)
        source = upper_bits + chosen_bit + lower_bits
    return source


def contract(left, right):
    return lax.dot_general(left, right, (((1,), (1,)), ((), ())), precision=lax.Precision.HIGHEST, preferred_element_type=jnp.float32)


def reference(state_real, state_imag, subsystem):
    source_map = insert_bits(subsystem, 2 ** SUB_LOCAL, COMPLEMENT)
    psi_real = state_real.reshape(N_DEV, AMPS_DEV)[:, source_map].reshape(SUB_DIM, COMPLEMENT)
    psi_imag = state_imag.reshape(N_DEV, AMPS_DEV)[:, source_map].reshape(SUB_DIM, COMPLEMENT)
    inverse_rest = 1.0 / COMPLEMENT
    rho_real = (contract(psi_real, psi_real) + contract(psi_imag, psi_imag)) * inverse_rest
    rho_imag = (contract(psi_imag, psi_real) - contract(psi_real, psi_imag)) * inverse_rest
    return rho_real, rho_imag
```

```python
import functools

import jax
import jax.numpy as jnp
from jax import lax
from jax.experimental import pallas as pl
from jax.experimental.pallas import tpu as pltpu
from jax.sharding import PartitionSpec as P

MESH = pl.DeviceIdType.MESH


def exchange_kernel(n, scale, sub_ref, re_hbm, im_hbm, out_ref, state, mixed, send, recv,
                    part_ref, pair_ref, rows_ref, load_sem, send_sem, recv_sem, own_sem,
                    pair_send, pair_recv, row_send, row_recv):
    me = lax.axis_index("dev")
    barrier = pltpu.get_barrier_semaphore()
    loads = [
        pltpu.make_async_copy(re_hbm, state.at[0], load_sem.at[0]),
        pltpu.make_async_copy(im_hbm, state.at[1], load_sem.at[1]),
    ]
    for load in loads:
        load.start()

    def greet(k, carry):
        pl.semaphore_signal(barrier, inc=1, device_id=(lax.rem(me + k, n),), device_id_type=MESH)
        return carry

    lax.fori_loop(1, n, greet, 0)
    vregs = state.shape[1]
    quarter = vregs // 4
    bits = vregs.bit_length() - 1
    width = vregs // n

    lane = lax.broadcasted_iota(jnp.int32, (8, 128), 1)
    sub = lax.broadcasted_iota(jnp.int32, (8, 128), 0)

    mid = sub_ref[1]
    lane_step = jnp.int32(1)
    for b in range(1, 7):
        lane_step = jnp.where(mid == b, 2**b, lane_step)
    top = 10 + bits - 1
    in_lane = (mid < 7) | (mid == top - 1)
    stride = jnp.int32(vregs // 8)
    for b in range(10, top - 1):
        stride = jnp.where(mid == b, 2 ** (b - 10), stride)
    stride = jnp.where(mid == 7, vregs // 4, stride)
    stride = jnp.where(mid == 9, vregs // 2, stride)
    fixed = mid == 8
    lane_on = jnp.where(in_lane, lane_step, 0)
    lane_hit = jnp.bitwise_and(lane, lane_on) != 0
    lane_keep = lane_hit | (jnp.where(in_lane, 0, 1) != jnp.bitwise_and(lane, 0))
    sub_on = jnp.where(fixed, 0, 2)
    sub_hit = jnp.bitwise_and(sub, sub_on) != 0
    sub_keep = sub_hit | (jnp.where(fixed, 1, 0) != jnp.bitwise_and(sub, 0))

    high4 = sub >= 4
    odd_sub = jnp.bitwise_and(sub, 1) != 0
    odd_lane = jnp.bitwise_and(lane, 1) != 0

    def swap(a, b, hit, keep, step, axis):
        size = (8, 128)[axis]
        back = size - step
        return (
            jnp.where(hit, pltpu.roll(b, step, axis), a),
            jnp.where(keep, b, pltpu.roll(a, back, axis)),
        )

    for load in loads:
        load.wait()

    def first_pass(v, carry):
        for c in range(2):
            x = [state[c, v + quarter * k] for k in range(4)]
            x[0], x[2] = swap(x[0], x[2], high4, high4, 4, 0)
            x[1], x[3] = swap(x[1], x[3], high4, high4, 4, 0)
            for k in (0, 2):
                a, b = swap(x[k], x[k + 1], odd_lane, odd_lane, 1, 1)
                x[k], x[k + 1] = swap(a, b, odd_sub, odd_sub, 1, 0)
            for k in range(4):
                mixed[c, v + quarter * k] = x[k]
        return carry

    lax.fori_loop(0, quarter, first_pass, 0, unroll=4)

    pl.semaphore_wait(barrier, n - 1)

    dests = max(1, 2 // width)
    pairs = max(1, width // 2)
    rounds = n // dests

    def second_pass(k, carry):
        at = lax.rem(me // dests + k, rounds)
        for c in range(2):
            for p in range(pairs):
                u = at * pairs + p
                low = jnp.bitwise_and(u, stride - 1)
                first = 2 * u - low
                a = mixed[c, first]
                b = mixed[c, first + stride]
                a, b = swap(a, b, lane_hit, lane_keep, lane_step, 1)
                a, b = swap(a, b, sub_hit, sub_keep, 2, 0)
                for w, value in enumerate((a, b)):
                    dest, tile = divmod(2 * p + w, width)
                    column = (c * width + tile) * 128
                    send[at * dests + dest, :, column : column + 128] = value
        for e in range(dests):
            j = at * dests + e

            @pl.when(j != me)
            def _():
                pltpu.make_async_remote_copy(
                    src_ref=send.at[j], dst_ref=recv.at[me], send_sem=send_sem,
                    recv_sem=recv_sem, device_id=(j,), device_id_type=MESH,
                ).start()

        return carry

    lax.fori_loop(1, rounds + 1, second_pass, 0)
    own = pltpu.make_async_copy(send.at[me], recv.at[me], own_sem)
    own.start()
    own.wait()
    others = pl.ds(0, n - 1)
    pltpu.make_async_copy(recv.at[others], recv.at[others], recv_sem).wait()

    full = 8 * n
    depth = width * 128
    block = min(full, 256)
    half_blocks = block // 16
    chips = n // 2

    def split(x):
        high = x.astype(jnp.bfloat16)
        return high, (x - high.astype(jnp.float32)).astype(jnp.bfloat16)

    def dot(x, y):
        return lax.dot_general(x, y, (((1,), (1,)), ((), ())), preferred_element_type=jnp.float32)

    right = recv[...].reshape(full, 2 * depth)
    right_h, right_l = split(right)

    def gram_block(i, carry):
        rows = recv[pl.ds(i * (block // 8), block // 8)].reshape(block, 2 * depth)
        turned = jnp.concatenate([rows[:, depth:], -rows[:, :depth]], axis=1)
        for c, left in enumerate((rows, turned)):
            left_h, left_l = split(left)
            result = dot(left_h, right_h) + (dot(left_h, right_l) + dot(left_l, right_h))
            result = result.reshape(half_blocks, 2, 8, full)
            for e in range(2):
                part_ref[e, pl.ds(i * half_blocks, half_blocks), :, c * full : (c + 1) * full] = result[:, e]
        return carry

    lax.fori_loop(0, full // block, gram_block, 0)

    core = lax.rem(me, 2)
    chip = me // 2
    other = 1 - core
    to_pair = pltpu.make_async_remote_copy(
        src_ref=part_ref.at[other], dst_ref=pair_ref, send_sem=pair_send, recv_sem=pair_recv,
        device_id=(2 * chip + other,), device_id_type=MESH,
    )
    to_pair.start()
    to_pair.wait_recv()

    def add_pair(k, carry):
        j = lax.rem(chip + k, chips)
        part_ref[core, j] = part_ref[core, j] + pair_ref[j]

        @pl.when(j != chip)
        def _():
            pltpu.make_async_remote_copy(
                src_ref=part_ref.at[core, j], dst_ref=rows_ref.at[chip], send_sem=row_send,
                recv_sem=row_recv, device_id=(2 * j + core,), device_id_type=MESH,
            ).start()

        return carry

    lax.fori_loop(1, chips + 1, add_pair, 0)
    rows_ref[chip] = part_ref[core, chip]
    rest = pl.ds(0, chips - 1)
    pltpu.make_async_copy(rows_ref.at[rest], rows_ref.at[rest], row_recv).wait()
    out_ref[...] = jnp.sum(rows_ref[...], axis=0) * scale
    pltpu.make_async_copy(send.at[others], send.at[others], send_sem).wait()
    to_pair.wait_send()
    pltpu.make_async_copy(rows_ref.at[rest], rows_ref.at[rest], row_send).wait()


def local(n, state_real, state_imag, subsystem):
    amps = state_real.shape[0]
    vregs = amps // 1024
    width = vregs // n
    full = 8 * n
    chunk = (n, 8, 2 * width * 128)
    out = pl.pallas_call(
        functools.partial(exchange_kernel, n, 8.0 / amps),
        out_shape=jax.ShapeDtypeStruct((8, 2 * full), jnp.float32),
        in_specs=[
            pl.BlockSpec(memory_space=pltpu.SMEM),
            pl.BlockSpec(memory_space=pl.ANY),
            pl.BlockSpec(memory_space=pl.ANY),
        ],
        out_specs=pl.BlockSpec(memory_space=pltpu.VMEM),
        scratch_shapes=[
            pltpu.VMEM((2, vregs, 8, 128), jnp.float32),
            pltpu.VMEM((2, vregs, 8, 128), jnp.float32),
            pltpu.VMEM(chunk, jnp.float32),
            pltpu.VMEM(chunk, jnp.float32),
            pltpu.VMEM((2, n // 2, 8, 2 * full), jnp.float32),
            pltpu.VMEM((n // 2, 8, 2 * full), jnp.float32),
            pltpu.VMEM((n // 2, 8, 2 * full), jnp.float32),
            pltpu.SemaphoreType.DMA((2,)),
        ]
        + [pltpu.SemaphoreType.DMA] * 7,
        compiler_params=pltpu.CompilerParams(
            collective_id=0, has_side_effects=True, vmem_limit_bytes=56 * 2**20
        ),
    )(subsystem, state_real.reshape(vregs, 8, 128), state_imag.reshape(vregs, 8, 128))
    return out[:, :full], out[:, full:]


def solution(mesh):
    return jax.shard_map(
        functools.partial(local, mesh.shape["dev"]),
        mesh=mesh,
        in_specs=(P("dev"), P("dev"), P()),
        out_specs=(P("dev", None), P("dev", None)),
        check_vma=False,
    )
```

```python
import functools

import jax
import jax.numpy as jnp
from jax import lax
from jax.experimental import pallas as pl
from jax.experimental.pallas import tpu as pltpu
from jax.sharding import PartitionSpec as P

MESH = pl.DeviceIdType.MESH


def exchange_kernel(n, scale, sub_hbm, re_hbm, im_hbm, out_ref, sub_ref, state, mixed, send, recv,
                    part_ref, pair_ref, rows_ref, load_sem, send_sem, recv_sem,
                    pair_send, pair_recv, row_send, row_recv):
    me = lax.axis_index("dev")
    barrier = pltpu.get_barrier_semaphore()

    def greet(k, carry):
        pl.semaphore_signal(
            barrier, inc=1, device_id=(jnp.bitwise_xor(me, n - k),), device_id_type=MESH
        )
        return carry

    lax.fori_loop(1, n, greet, 0)
    loads = [
        pltpu.make_async_copy(sub_hbm, sub_ref, load_sem.at[2]),
        pltpu.make_async_copy(re_hbm, state.at[0], load_sem.at[0]),
        pltpu.make_async_copy(im_hbm, state.at[1], load_sem.at[1]),
    ]
    for load in loads:
        load.start()
    vregs = state.shape[1]
    quarter = vregs // 4
    bits = vregs.bit_length() - 1
    width = vregs // n

    for load in loads:
        load.wait()

    lane = lax.broadcasted_iota(jnp.int32, (8, 128), 1)
    sub = lax.broadcasted_iota(jnp.int32, (8, 128), 0)

    mid = sub_ref[1]
    lane_step = jnp.int32(1)
    for b in range(1, 7):
        lane_step = jnp.where(mid == b, 2**b, lane_step)
    top = 10 + bits - 1
    in_lane = (mid < 7) | (mid == top - 1)
    stride = jnp.int32(vregs // 8)
    for b in range(10, top - 1):
        stride = jnp.where(mid == b, 2 ** (b - 10), stride)
    stride = jnp.where(mid == 7, vregs // 4, stride)
    stride = jnp.where(mid == 9, vregs // 2, stride)
    fixed = mid == 8
    lane_on = jnp.where(in_lane, lane_step, 0)
    lane_hit = jnp.bitwise_and(lane, lane_on) != 0
    lane_keep = lane_hit | (jnp.where(in_lane, 0, 1) != jnp.bitwise_and(lane, 0))
    sub_on = jnp.where(fixed, 0, 2)
    sub_hit = jnp.bitwise_and(sub, sub_on) != 0
    sub_keep = sub_hit | (jnp.where(fixed, 1, 0) != jnp.bitwise_and(sub, 0))

    high4 = sub >= 4
    odd_sub = jnp.bitwise_and(sub, 1) != 0
    odd_lane = jnp.bitwise_and(lane, 1) != 0

    def swap(a, b, hit, keep, step, axis):
        size = (8, 128)[axis]
        back = size - step
        return (
            jnp.where(hit, pltpu.roll(b, step, axis), a),
            jnp.where(keep, b, pltpu.roll(a, back, axis)),
        )

    def first_pass(v, carry):
        for c in range(2):
            x = [state[c, v + quarter * k] for k in range(4)]
            x[0], x[2] = swap(x[0], x[2], high4, high4, 4, 0)
            x[1], x[3] = swap(x[1], x[3], high4, high4, 4, 0)
            for k in (0, 2):
                a, b = swap(x[k], x[k + 1], odd_lane, odd_lane, 1, 1)
                x[k], x[k + 1] = swap(a, b, odd_sub, odd_sub, 1, 0)
            for k in range(4):
                mixed[c, v + quarter * k] = x[k]
        return carry

    lax.fori_loop(0, quarter, first_pass, 0, unroll=4)

    dests = max(1, 2 // width)
    pairs = max(1, width // 2)
    rounds = n // dests

    def second_pass(at, carry):
        for c in range(2):
            for p in range(pairs):
                u = at * pairs + p
                low = jnp.bitwise_and(u, stride - 1)
                first = 2 * u - low
                a = mixed[c, first]
                b = mixed[c, first + stride]
                a, b = swap(a, b, lane_hit, lane_keep, lane_step, 1)
                a, b = swap(a, b, sub_hit, sub_keep, 2, 0)
                for w, value in enumerate((a, b)):
                    dest, tile = divmod(2 * p + w, width)
                    column = (c * width + tile) * 128
                    send[at * dests + dest, :, column : column + 128] = value
        return carry

    lax.fori_loop(0, rounds, second_pass, 0, unroll=4)

    core = lax.rem(me, 2)
    other = 1 - core
    chip = me // 2
    chips = n // 2
    pl.semaphore_wait(barrier, n - 1)

    def send_chunk(k, carry):
        j = jnp.bitwise_xor(me, n - k)
        pltpu.make_async_remote_copy(
            src_ref=send.at[j], dst_ref=recv.at[chip, core], send_sem=send_sem,
            recv_sem=recv_sem, device_id=(j,), device_id_type=MESH,
        ).start()
        return carry

    lax.fori_loop(1, n, send_chunk, 0)
    pltpu.make_async_copy(send.at[me], recv.at[chip, core], recv_sem).start()
    pltpu.make_async_copy(recv, recv, recv_sem).wait()

    full = 8 * n
    depth = width * 128
    block = min(full // 2, 256)
    blocks = full // 2 // block
    group = block // 8

    def split(x):
        high = x.astype(jnp.bfloat16)
        return high, (x - high.astype(jnp.float32)).astype(jnp.bfloat16)

    def dot(x, y):
        return lax.dot_general(x, y, (((1,), (1,)), ((), ())), preferred_element_type=jnp.float32)

    right_h, right_l = split(recv[...].reshape(full, 2 * depth))

    def gram(side):
        def gram_block(i, carry):
            chunk = pl.ds(i * group, group)
            left = recv[chunk, side].reshape(block, 2 * depth)
            turned = jnp.concatenate([left[:, depth:], -left[:, :depth]], axis=1)
            left_h, left_l = split(jnp.concatenate([left, turned], axis=0))
            result = dot(left_h, right_h) + (dot(left_h, right_l) + dot(left_l, right_h))
            for c in range(2):
                part_ref[side, chunk, :, c * full : (c + 1) * full] = result[
                    c * block : (c + 1) * block
                ].reshape(group, 8, full)
            return carry

        lax.fori_loop(0, blocks, gram_block, 0)

    to_pair = pltpu.make_async_remote_copy(
        src_ref=part_ref.at[other], dst_ref=pair_ref, send_sem=pair_send, recv_sem=pair_recv,
        device_id=(2 * chip + other,), device_id_type=MESH,
    )
    gram(other)
    to_pair.start()
    gram(core)
    to_pair.wait_recv()

    def add_pair(k, carry):
        j = jnp.bitwise_xor(chip, chips - k)
        part_ref[core, j] = part_ref[core, j] + pair_ref[j]
        pltpu.make_async_remote_copy(
            src_ref=part_ref.at[core, j], dst_ref=rows_ref.at[chip], send_sem=row_send,
            recv_sem=row_recv, device_id=(2 * j + core,), device_id_type=MESH,
        ).start()
        return carry

    lax.fori_loop(1, chips, add_pair, 0)
    rows_ref[chip] = part_ref[core, chip] + pair_ref[chip]
    rest = pl.ds(0, chips - 1)
    pltpu.make_async_copy(rows_ref.at[rest], rows_ref.at[rest], row_recv).wait()
    out_ref[...] = jnp.sum(rows_ref[...], axis=0) * scale
    others = send.at[pl.ds(0, n - 1)]
    pltpu.make_async_copy(others, others, send_sem).wait()
    to_pair.wait_send()
    pltpu.make_async_copy(rows_ref.at[rest], rows_ref.at[rest], row_send).wait()


def local(n, state_real, state_imag, subsystem):
    amps = state_real.shape[0]
    vregs = amps // 1024
    width = vregs // n
    full = 8 * n
    chunk = (n, 8, 2 * width * 128)
    out = pl.pallas_call(
        functools.partial(exchange_kernel, n, 8.0 / amps),
        out_shape=jax.ShapeDtypeStruct((8, 2 * full), jnp.float32),
        in_specs=[
            pl.BlockSpec(memory_space=pl.ANY),
            pl.BlockSpec(memory_space=pl.ANY),
            pl.BlockSpec(memory_space=pl.ANY),
        ],
        out_specs=pl.BlockSpec(memory_space=pltpu.VMEM),
        scratch_shapes=[
            pltpu.SMEM((3,), jnp.int32),
            pltpu.VMEM((2, vregs, 8, 128), jnp.float32),
            pltpu.VMEM((2, vregs, 8, 128), jnp.float32),
            pltpu.VMEM(chunk, jnp.float32),
            pltpu.VMEM((n // 2, 2) + chunk[1:], jnp.float32),
            pltpu.VMEM((2, n // 2, 8, 2 * full), jnp.float32),
            pltpu.VMEM((n // 2, 8, 2 * full), jnp.float32),
            pltpu.VMEM((n // 2, 8, 2 * full), jnp.float32),
            pltpu.SemaphoreType.DMA((3,)),
        ]
        + [pltpu.SemaphoreType.DMA] * 6,
        compiler_params=pltpu.CompilerParams(
            collective_id=0, has_side_effects=True, vmem_limit_bytes=56 * 2**20
        ),
    )(subsystem, state_real.reshape(vregs, 8, 128), state_imag.reshape(vregs, 8, 128))
    return out[:, :full], out[:, full:]


def solution(mesh):
    return jax.shard_map(
        functools.partial(local, mesh.shape["dev"]),
        mesh=mesh,
        in_specs=(P("dev"), P("dev"), P()),
        out_specs=(P("dev", None), P("dev", None)),
        check_vma=False,
    )
```

```python
import functools

import jax
import jax.numpy as jnp
from jax import lax
from jax.experimental import pallas as pl
from jax.experimental.pallas import tpu as pltpu
from jax.sharding import PartitionSpec as P

MESH = pl.DeviceIdType.MESH


def exchange_kernel(n, sub_hbm, re_hbm, im_hbm, rows_ref, sub_ref, state, mixed, send, recv,
                    part_ref, pair_ref, load_sem, send_sem, recv_sem,
                    pair_send, pair_recv, row_send, row_recv):
    me = lax.axis_index("dev")
    barrier = pltpu.get_barrier_semaphore()

    def greet(k, carry):
        pl.semaphore_signal(
            barrier, inc=1, device_id=(jnp.bitwise_xor(me, n - k),), device_id_type=MESH
        )
        return carry

    lax.fori_loop(1, n, greet, 0)
    loads = [
        pltpu.make_async_copy(sub_hbm, sub_ref, load_sem.at[2]),
        pltpu.make_async_copy(re_hbm, state.at[0], load_sem.at[0]),
        pltpu.make_async_copy(im_hbm, state.at[1], load_sem.at[1]),
    ]
    for load in loads:
        load.start()
    vregs = state.shape[1]
    quarter = vregs // 4
    bits = vregs.bit_length() - 1
    width = vregs // n

    for load in loads:
        load.wait()

    lane = lax.broadcasted_iota(jnp.int32, (8, 128), 1)
    sub = lax.broadcasted_iota(jnp.int32, (8, 128), 0)

    mid = sub_ref[1]
    lane_step = jnp.int32(1)
    for b in range(1, 7):
        lane_step = jnp.where(mid == b, 2**b, lane_step)
    top = 10 + bits - 1
    in_lane = (mid < 7) | (mid == top - 1)
    stride = jnp.int32(vregs // 8)
    for b in range(10, top - 1):
        stride = jnp.where(mid == b, 2 ** (b - 10), stride)
    stride = jnp.where(mid == 7, vregs // 4, stride)
    stride = jnp.where(mid == 9, vregs // 2, stride)
    fixed = mid == 8
    lane_on = jnp.where(in_lane, lane_step, 0)
    lane_hit = jnp.bitwise_and(lane, lane_on) != 0
    lane_keep = lane_hit | (jnp.where(in_lane, 0, 1) != jnp.bitwise_and(lane, 0))
    sub_on = jnp.where(fixed, 0, 2)
    sub_hit = jnp.bitwise_and(sub, sub_on) != 0
    sub_keep = sub_hit | (jnp.where(fixed, 1, 0) != jnp.bitwise_and(sub, 0))

    high4 = sub >= 4
    odd_sub = jnp.bitwise_and(sub, 1) != 0
    odd_lane = jnp.bitwise_and(lane, 1) != 0

    def swap(a, b, hit, keep, step, axis):
        size = (8, 128)[axis]
        back = size - step
        return (
            jnp.where(hit, pltpu.roll(b, step, axis), a),
            jnp.where(keep, b, pltpu.roll(a, back, axis)),
        )

    def first_pass(v, carry):
        for c in range(2):
            x = [state[c, v + quarter * k] for k in range(4)]
            x[0], x[2] = swap(x[0], x[2], high4, high4, 4, 0)
            x[1], x[3] = swap(x[1], x[3], high4, high4, 4, 0)
            for k in (0, 2):
                a, b = swap(x[k], x[k + 1], odd_lane, odd_lane, 1, 1)
                x[k], x[k + 1] = swap(a, b, odd_sub, odd_sub, 1, 0)
            for k in range(4):
                mixed[c, v + quarter * k] = x[k]
        return carry

    lax.fori_loop(0, quarter, first_pass, 0, unroll=4)

    dests = max(1, 2 // width)
    pairs = max(1, width // 2)
    rounds = n // dests

    def second_pass(at, carry):
        for c in range(2):
            for p in range(pairs):
                u = at * pairs + p
                low = jnp.bitwise_and(u, stride - 1)
                first = 2 * u - low
                a = mixed[c, first]
                b = mixed[c, first + stride]
                a, b = swap(a, b, lane_hit, lane_keep, lane_step, 1)
                a, b = swap(a, b, sub_hit, sub_keep, 2, 0)
                for w, value in enumerate((a, b)):
                    dest, tile = divmod(2 * p + w, width)
                    column = (c * width + tile) * 128
                    send[at * dests + dest, :, column : column + 128] = value
        return carry

    lax.fori_loop(0, rounds, second_pass, 0, unroll=4)

    core = lax.rem(me, 2)
    other = 1 - core
    chip = me // 2
    chips = n // 2
    pl.semaphore_wait(barrier, n - 1)

    def send_chunk(k, carry):
        j = jnp.bitwise_xor(me, n - k)
        pltpu.make_async_remote_copy(
            src_ref=send.at[j], dst_ref=recv.at[chip, core], send_sem=send_sem,
            recv_sem=recv_sem, device_id=(j,), device_id_type=MESH,
        ).start()
        return carry

    lax.fori_loop(1, n, send_chunk, 0)
    pltpu.make_async_copy(send.at[me], recv.at[chip, core], recv_sem).start()
    pltpu.make_async_copy(recv, recv, recv_sem).wait()

    full = 8 * n
    depth = width * 128
    block = min(full // 2, 256)
    blocks = full // 2 // block
    group = block // 8

    def split(x):
        high = x.astype(jnp.bfloat16)
        return high, (x - high.astype(jnp.float32)).astype(jnp.bfloat16)

    def dot(x, y):
        return lax.dot_general(x, y, (((1,), (1,)), ((), ())), preferred_element_type=jnp.float32)

    right_h, right_l = split(recv[...].reshape(full, 2 * depth))

    def gram(side):
        def gram_block(i, carry):
            chunk = pl.ds(i * group, group)
            left = recv[chunk, side].reshape(block, 2 * depth)
            turned = jnp.concatenate([left[:, depth:], -left[:, :depth]], axis=1)
            left_h, left_l = split(jnp.concatenate([left, turned], axis=0))
            result = dot(left_h, right_h) + (dot(left_h, right_l) + dot(left_l, right_h))
            for c in range(2):
                part_ref[side, chunk, :, c * full : (c + 1) * full] = result[
                    c * block : (c + 1) * block
                ].reshape(group, 8, full)
            return carry

        lax.fori_loop(0, blocks, gram_block, 0)

    to_pair = pltpu.make_async_remote_copy(
        src_ref=part_ref.at[other], dst_ref=pair_ref, send_sem=pair_send, recv_sem=pair_recv,
        device_id=(2 * chip + other,), device_id_type=MESH,
    )
    gram(other)
    to_pair.start()
    gram(core)
    to_pair.wait_recv()

    def add_pair(k, carry):
        j = jnp.bitwise_xor(chip, chips - k)
        part_ref[core, j] = part_ref[core, j] + pair_ref[j]
        pltpu.make_async_remote_copy(
            src_ref=part_ref.at[core, j], dst_ref=rows_ref.at[chip], send_sem=row_send,
            recv_sem=row_recv, device_id=(2 * j + core,), device_id_type=MESH,
        ).start()
        return carry

    lax.fori_loop(1, chips, add_pair, 0)
    part_ref[core, chip] = part_ref[core, chip] + pair_ref[chip]
    pltpu.make_async_copy(part_ref.at[core, chip], rows_ref.at[chip], row_recv).start()
    rest = pl.ds(0, chips - 1)
    pltpu.make_async_copy(rows_ref, rows_ref, row_recv).wait()
    others = send.at[pl.ds(0, n - 1)]
    pltpu.make_async_copy(others, others, send_sem).wait()
    to_pair.wait_send()
    pltpu.make_async_copy(rows_ref.at[rest], rows_ref.at[rest], row_send).wait()


def local(n, state_real, state_imag, subsystem):
    amps = state_real.shape[0]
    vregs = amps // 1024
    width = vregs // n
    full = 8 * n
    chunk = (n, 8, 2 * width * 128)
    out = pl.pallas_call(
        functools.partial(exchange_kernel, n),
        out_shape=jax.ShapeDtypeStruct((n // 2, 8, 2 * full), jnp.float32),
        in_specs=[
            pl.BlockSpec(memory_space=pl.ANY),
            pl.BlockSpec(memory_space=pl.ANY),
            pl.BlockSpec(memory_space=pl.ANY),
        ],
        out_specs=pl.BlockSpec(memory_space=pl.ANY),
        scratch_shapes=[
            pltpu.SMEM((3,), jnp.int32),
            pltpu.VMEM((2, vregs, 8, 128), jnp.float32),
            pltpu.VMEM((2, vregs, 8, 128), jnp.float32),
            pltpu.VMEM(chunk, jnp.float32),
            pltpu.VMEM((n // 2, 2) + chunk[1:], jnp.float32),
            pltpu.VMEM((2, n // 2, 8, 2 * full), jnp.float32),
            pltpu.VMEM((n // 2, 8, 2 * full), jnp.float32),
            pltpu.SemaphoreType.DMA((3,)),
        ]
        + [pltpu.SemaphoreType.DMA] * 6,
        compiler_params=pltpu.CompilerParams(
            collective_id=0, has_side_effects=True, vmem_limit_bytes=56 * 2**20
        ),
    )(subsystem, state_real.reshape(vregs, 8, 128), state_imag.reshape(vregs, 8, 128))
    total = jnp.sum(out, axis=0) * (8.0 / amps)
    return total[:, :full], total[:, full:]


def solution(mesh):
    return jax.shard_map(
        functools.partial(local, mesh.shape["dev"]),
        mesh=mesh,
        in_specs=(P("dev"), P("dev"), P()),
        out_specs=(P("dev", None), P("dev", None)),
        check_vma=False,
    )
```
